256 devices in a mesh: rows: 64 (over z, x, core), feat: 4 (over y).
Axes of the slice: x: 4, y: 4, z: 8, core: 2. Of those that a mesh axis runs over, the one named last changes fastest.
Arguments:
- samples: float32 [65536, 440], P(('rows', 'feat')), may hold values from -6 to 6
- residual: float32 [65536, 147], P(('rows', 'feat')), may hold values from -4 to 4
- projections: float32 [8, 440, 1024], P('feat'), may hold values from -0.4375 to 0.4375
- phases: float32 [8, 1024], P('feat'), may hold values from 0 to 6.2831855
- weights: float32 [8, 1024, 147], P('feat'), may hold values from -4 to 4
- block_order: int32 [8], replicated, may hold values from 0 to 7, each once
Outputs:
- residual_out: float32 [65536, 147], P(('rows', 'feat'))
- new_weights: float32 [1, 1024, 147], replicated
The draws below stay inside these ranges and needn't reach their ends.
Inputs may be any that keep to these rules, and one draw needn't show every extreme that they name: Block k is held by index k // 2 of feat; the blocks updated are those of the first 1 entries of block_order.
All inputs are finite; a program needn't handle non-finite values.
Results may differ from the reference program's by a relative error of at most 0.0003.
Values sent between devices are 32-bit elements; how exact they have to be, the bound alone decides.
No kernel may reach another device: no remote copies, remote signals or barrier semaphores. Data moves between devices by JAX's collectives and lax.ppermute only.
A program may use at most 128 MiB of HBM per device.

```python
import jax
import jax.numpy as jnp
from jax import lax

D_IN = 440
BLK = 1024
OUT = 147
UPDATES = 1
BLOCKS = 8
TOTAL_ROWS = 65536


def shared_draw(key):
    inner = jax.random.fold_in(key, 7)
    first, second, third = jax.random.split(inner, 3)
    samples = jnp.clip(jax.random.normal(first, (TOTAL_ROWS, D_IN), jnp.float32), -6.0, 6.0)
    mixing = jax.random.normal(second, (D_IN, OUT), jnp.float32) / jnp.sqrt(jnp.float32(D_IN))
    signal = 1.5 * jnp.sin(jnp.dot(samples, mixing, precision=lax.Precision.HIGHEST))
    noise = 0.5 * jnp.clip(jax.random.normal(third, (TOTAL_ROWS, OUT), jnp.float32), -4.0, 4.0)
    residual = signal + noise
    return (samples, jnp.clip(residual, -4.0, 4.0))


def draw_samples(key, part):
    return shared_draw(key)[0]


def draw_residual(key, part):
    return shared_draw(key)[1]


def level_of(own_key, dims, cuts, smallest, top_value):
    level, own = 1.0, jax.random.fold_in(own_key, 6)
    for position, shards_of in cuts:
        heights = jnp.exp(jax.random.uniform(jax.random.fold_in(own, position), (shards_of,), jnp.float32, smallest / len(cuts), top_value / len(cuts)))
        level = level * jnp.repeat(heights, dims[position] // shards_of).reshape([-1 if axis == position else 1 for axis in range(len(dims))])
    return level


def scatter_about(key, shape, width, most, shards=(), held_as=jnp.bfloat16):
    array = jax.random.normal(key, shape, jnp.float32) * width
    if len(shards) > 0:
        array = level_of(key, shape, shards, -0.22, 0.18) * array
    return jnp.clip(array, min=-most, max=most).astype(held_as)


def setup_inputs(seed: int = 0) -> dict:
    arg_keys = jax.random.split(jax.random.key(seed), 7)
    return {
        "samples": draw_samples(jax.random.fold_in(arg_keys[6], 71), 0),
        "residual": draw_residual(jax.random.fold_in(arg_keys[6], 71), 0),
        "projections": scatter_about(arg_keys[2], (BLOCKS, D_IN, BLK), (D_IN // 2) ** -0.5, 0.4375, ((0, 4),), jnp.float32),
        "phases": jnp.clip(6.2831855 * jax.random.uniform(arg_keys[3], (BLOCKS, BLK), jnp.float32) ** level_of(arg_keys[3], (BLOCKS, BLK), ((0, 4),), -0.2, 0.2), 0.0, 6.2831855),
        "weights": scatter_about(arg_keys[4], (BLOCKS, BLK, OUT), 0.3, 4.0, ((0, 4),), jnp.float32),
        "block_order": jax.random.permutation(arg_keys[5], BLOCKS).astype(jnp.int32),
    }


root_two = 1.4142135623730951
penalty = 0.05

def features_of(samples, basis_block, phase_block):
    projected = jnp.dot(samples.astype(jnp.float32), basis_block.astype(jnp.float32), precision=lax.Precision.HIGHEST, preferred_element_type=jnp.float32)
    return root_two * jnp.cos(projected + phase_block)

def reference(samples, residual, projections, phases, weights, block_order):
    results = []
    for update in range(UPDATES):
        block_id = block_order[update].astype(jnp.int32)
        basis_block = lax.dynamic_index_in_dim(projections, block_id, 0, False)
        phase_block = lax.dynamic_index_in_dim(phases, block_id, 0, False)
        old_weights = lax.dynamic_index_in_dim(weights, block_id, 0, False)
        features = features_of(samples, basis_block, phase_block)
        gram_matrix = jnp.dot(features.T.astype(jnp.float32), features.astype(jnp.float32), precision=lax.Precision.HIGHEST, preferred_element_type=jnp.float32) / TOTAL_ROWS
        cross_term = jnp.dot(features.T.astype(jnp.float32), residual.astype(jnp.float32), precision=lax.Precision.HIGHEST, preferred_element_type=jnp.float32) / TOTAL_ROWS
        system = gram_matrix + penalty * jnp.eye(BLK, dtype=jnp.float32)
        factor = jnp.linalg.cholesky(system)
        change = jax.scipy.linalg.cho_solve((factor, True), cross_term - penalty * old_weights)
        results.append(old_weights + change)
        residual = residual - jnp.dot(features.astype(jnp.float32), change.astype(jnp.float32), precision=lax.Precision.HIGHEST, preferred_element_type=jnp.float32)
    return (residual, jnp.stack(results))
```

```python
import functools

import jax
import jax.numpy as jnp
from jax import lax
from jax.experimental import pallas as pl
from jax.experimental.pallas import tpu as pltpu
from jax.sharding import Mesh
from jax.sharding import PartitionSpec as P

ROWS = ("z", "x", "core")
ROWS_FEAT = ("z", "x", "core", "feat")
HIGHEST = lax.Precision.HIGHEST
F32 = jnp.float32

root_two = 1.4142135623730951
penalty = 0.05

LANES = 128
CHUNK = 80
PHASE_ROW = 440
WEIGHT_ROW = 448
BLOCK_ROWS = 640
EXTRA = 152
HALF = 3072

INTERPRET = False


def call(kernel, out_shape, *args, scalars=0, scratch=(), cost=None):
    specs = [pl.BlockSpec(memory_space=pltpu.SMEM)] * scalars
    specs += [pl.BlockSpec(memory_space=pltpu.VMEM)] * (len(args) - scalars)
    outs = jax.tree.map(lambda _: pl.BlockSpec(memory_space=pltpu.VMEM), out_shape)
    return pl.pallas_call(
        kernel,
        out_shape=out_shape,
        in_specs=specs,
        out_specs=outs,
        scratch_shapes=list(scratch),
        cost_estimate=cost,
        interpret=INTERPRET,
    )(*args)


def rows_of(count):
    return jax.ShapeDtypeStruct((count, LANES), F32)


def shifted(x, axis, by):
    size = lax.axis_size(axis)
    return lax.ppermute(x, axis, [(i, (i + by) % size) for i in range(size)])


def from_others(pieces, axis):
    return [shifted(piece, axis, s) for s, piece in enumerate(pieces, 1)]


def to_others(piece, axis):
    return [shifted(piece, axis, s) for s in range(1, lax.axis_size(axis))]


def wrapped(value, size):
    return lax.rem(value + size, size)


def index_of(axis):
    return lax.axis_index(axis).astype(jnp.int32)


def placed(me, piece, others):
    count, rows = len(others) + 1, piece.shape[0]

    def kernel(me_ref, *refs):
        out_ref = refs[-1]
        for s in range(count):
            at = wrapped(me_ref[0] - s, count)
            out_ref[pl.ds(pl.multiple_of(at * rows, 8), rows), :] = refs[s][...]

    return call(kernel, rows_of(count * rows), me.reshape(1), piece, *others, scalars=1)


def placed_pair(mes, pair, others):
    count, rows = len(others[0]) + 1, pair[0].shape[0]

    def kernel(me_ref, *refs):
        ins, outs = refs[:-2], refs[-2:]
        for c in range(2):
            for s in range(count):
                at = wrapped(me_ref[c] - s, count)
                outs[c][pl.ds(pl.multiple_of(at * rows, 8), rows), :] = ins[c * count + s][...]

    args = [x for own, rest in zip(pair, others) for x in (own, *rest)]
    return call(
        kernel, (rows_of(count * rows),) * 2, jnp.stack(mes), *args, scalars=1
    )


def chunk_of(projections, phases, weights, block_id):
    per_device = projections.shape[0]
    depth, width = projections.shape[1], projections.shape[2]
    outs = weights.shape[2]
    slot = block_id % per_device
    column = (index_of("core") * lax.axis_size("x") + index_of("x")) * LANES
    basis = lax.dynamic_slice(projections, (slot, 0, column), (1, depth, LANES))[0]
    phase = lax.dynamic_slice(phases, (slot, column), (1, LANES))
    old = lax.dynamic_slice(weights, (slot, column, 0), (1, LANES, outs))[0].T
    stacked = jnp.concatenate(
        [
            basis,
            phase,
            jnp.zeros((WEIGHT_ROW - depth - 1, LANES), F32),
            old,
            jnp.zeros((BLOCK_ROWS - WEIGHT_ROW - outs, LANES), F32),
        ]
    )
    return lax.dynamic_slice(stacked, (index_of("z") * CHUNK, 0), (CHUNK, LANES))


def updated_block(projections, phases, weights, block_id):
    per_device = projections.shape[0]
    chunk = chunk_of(projections, phases, weights, block_id)
    feat = index_of("feat")
    distance = wrapped(feat - block_id // per_device, lax.axis_size("feat"))
    chosen = chunk
    for s, other in enumerate(to_others(chunk, "feat"), 1):
        chosen = jnp.where(distance == s, other, chosen)
    part = placed(index_of("z"), chosen, to_others(chosen, "z"))
    part = placed(index_of("x"), part, to_others(part, "x"))
    return placed(index_of("core"), part, to_others(part, "core"))


def cosine(x):
    turns = jnp.round(x * 0.15915494309189535)
    rest = (x - turns * 6.28125) - turns * 0.0019353071795864769
    sq = rest * rest * 0.25
    c = 2.08767569878681e-09
    for term in (
        -2.755731922398589e-07,
        2.48015873015873e-05,
        -0.001388888888888889,
        0.041666666666666664,
        -0.5,
        1.0,
    ):
        c = c * sq + term
    return 2.0 * (c * c) - 1.0


def products_kernel(core_ref, samples_ref, block_ref, residual_ref, features_ref, keep_ref, send_ref, turned, packed):
    blocks = features_ref.shape[1] // LANES
    depth = samples_ref.shape[1]
    total = blocks * LANES + EXTRA
    samples = samples_ref[...]
    for k in range(blocks):
        basis = block_ref[k * BLOCK_ROWS : k * BLOCK_ROWS + depth, :]
        phase = block_ref[k * BLOCK_ROWS + PHASE_ROW : k * BLOCK_ROWS + PHASE_ROW + 1, :]
        projected = jnp.dot(samples, basis, precision=HIGHEST, preferred_element_type=F32)
        features = root_two * cosine(projected + phase)
        features_ref[:, k * LANES : (k + 1) * LANES] = features
        turned[k * LANES : (k + 1) * LANES, :] = features.T
    turned[blocks * LANES :, :] = residual_ref[...].T[:EXTRA, :]
    at = 0
    for k in range(blocks):
        count = total - k * LANES
        packed[at : at + count, :] = jnp.dot(
            turned[k * LANES :, :],
            features_ref[:, k * LANES : (k + 1) * LANES],
            precision=HIGHEST,
            preferred_element_type=F32,
        )
        at += count
    packed[at:, :] = jnp.zeros((packed.shape[0] - at, LANES), F32)
    mine = pl.multiple_of(core_ref[0] * HALF, 8)
    theirs = pl.multiple_of((1 - core_ref[0]) * HALF, 8)
    keep_ref[...] = packed[pl.ds(mine, HALF), :]
    send_ref[...] = packed[pl.ds(theirs, HALF), :]


def products(samples, block, residual):
    rows, width = samples.shape[0], block.shape[0] // BLOCK_ROWS * LANES
    residual = jnp.pad(residual, ((0, 0), (0, 2 * LANES - residual.shape[1])))
    return call(
        products_kernel,
        (jax.ShapeDtypeStruct((rows, width), F32), rows_of(HALF), rows_of(HALF)),
        index_of("core").reshape(1),
        samples,
        block,
        residual,
        scalars=1,
        scratch=(pltpu.VMEM((width + EXTRA, rows), F32), pltpu.VMEM((2 * HALF, LANES), F32)),
    )


def summed_split(mes, groups, parts):
    joined = sum(group[0].shape[0] for group in groups)
    share = joined // len(mes)
    rows = share // parts
    sizes = [len(group) for group in groups]

    def kernel(me_ref, *refs):
        count = sum(sizes)
        ins, outs, scratch = refs[:count], refs[count:-1], refs[-1]
        first = at = 0
        for size in sizes:
            acc = ins[first][...]
            for ref in ins[first + 1 : first + size]:
                acc = acc + ref[...]
            scratch[at : at + acc.shape[0], :] = acc
            at += acc.shape[0]
            first += size
        for c in range(len(mes)):
            for s in range(parts):
                piece = wrapped(me_ref[c] + s, parts)
                start = pl.multiple_of(c * share + piece * rows, 8)
                outs[c * parts + s][...] = scratch[pl.ds(start, rows), :]

    outs = call(
        kernel,
        (rows_of(rows),) * (parts * len(mes)),
        jnp.stack(mes),
        *[x for group in groups for x in group],
        scalars=1,
        scratch=(pltpu.VMEM((joined, LANES), F32),),
    )
    return [outs[c * parts : (c + 1) * parts] for c in range(len(mes))]


def added(arrays):
    def kernel(*refs):
        acc = refs[0][...]
        for ref in refs[1:-1]:
            acc = acc + ref[...]
        refs[-1][...] = acc

    return call(kernel, rows_of(arrays[0].shape[0]), *arrays)


def total_of(keep, send):
    x, y, z = index_of("x"), index_of("feat"), index_of("z")
    halves = [[keep, *from_others([send], "core")]]
    a, b = summed_split((x, y), halves, lax.axis_size("x"))
    a = [a[0], *from_others(a[1:], "x")]
    b = [b[0], *from_others(b[1:], "feat")]
    a, b = summed_split((y, x), (a, b), lax.axis_size("x"))
    a = [a[0], *from_others(a[1:], "feat")]
    b = [b[0], *from_others(b[1:], "x")]
    (c,) = summed_split((z,), (a, b), lax.axis_size("z"))
    mine = added([c[0], *from_others(c[1:], "z")])
    both = placed(z, mine, to_others(mine, "z"))
    a, b = both[: both.shape[0] // 2], both[both.shape[0] // 2 :]
    a, b = placed_pair((y, x), (a, b), (to_others(a, "feat"), to_others(b, "x")))
    a, b = placed_pair((x, y), (a, b), (to_others(a, "x"), to_others(b, "feat")))
    half = jnp.concatenate([a, b])
    return half, shifted(half, "core", 1)


def across_sublanes(tile, row):
    return jnp.broadcast_to(tile[row : row + 1, :], tile.shape)


def inverse_factor(source, target):
    tiles = LANES // 8
    lane = lax.broadcasted_iota(jnp.int32, (8, LANES), 1)
    sub = lax.broadcasted_iota(jnp.int32, (8, LANES), 0)
    rows = [source[8 * v : 8 * v + 8, :] for v in range(tiles)]
    for b in range(tiles):
        inside = (lane >= 8 * b) & (lane < 8 * b + 8)
        tile = rows[b]
        columns = [
            jnp.broadcast_to(tile[:, 8 * b + q : 8 * b + q + 1], (8, LANES)) for q in range(8)
        ]
        tile = jnp.where(inside, jnp.where(lane == 8 * b + sub, 1.0, 0.0), tile)
        pivots = jnp.ones((8, LANES), F32)
        inverses, multiples, tops = [], [], []
        for q in range(8):
            pivot = across_sublanes(columns[q], q)
            pivots = jnp.where(sub == q, pivot, pivots)
            inverse = 1.0 / pivot
            factor = jnp.where(sub > q, columns[q] * inverse, 0.0)
            multiple = {}
            for later in range(q + 1, 8):
                multiple[later] = across_sublanes(columns[later], q)
                columns[later] = columns[later] - factor * multiple[later]
            top = across_sublanes(tile, q)
            tile = tile - factor * top
            inverses.append(inverse)
            multiples.append(multiple)
            tops.append(top)
        target[8 * b : 8 * b + 8, :] = jnp.where(
            lane <= 8 * b + sub, tile * lax.rsqrt(pivots), 0.0
        )
        for v in range(b + 1, tiles):
            below = rows[v]
            columns = [
                jnp.broadcast_to(below[:, 8 * b + q : 8 * b + q + 1], (8, LANES)) for q in range(8)
            ]
            below = jnp.where(inside, 0.0, below)
            for q in range(8):
                factor = columns[q] * inverses[q]
                for later in range(q + 1, 8):
                    columns[later] = columns[later] - factor * multiples[q][later]
                below = below - factor * tops[q]
            rows[v] = below


def dot_nt(a, b):
    return lax.dot_general(
        a, b, (((1,), (1,)), ((), ())), precision=HIGHEST, preferred_element_type=F32
    )


def solve_kernel(total_rows, core_ref, mine_ref, theirs_ref, block_ref, change_ref, new_ref, packed, lower, inverse, corner):
    width = change_ref.shape[1]
    blocks = width // LANES
    total = width + EXTRA
    packed[pl.ds(pl.multiple_of(core_ref[0] * HALF, 8), HALF), :] = mine_ref[...]
    packed[pl.ds(pl.multiple_of((1 - core_ref[0]) * HALF, 8), HALF), :] = theirs_ref[...]
    starts = [k * total - LANES * (k * (k - 1) // 2) for k in range(blocks)]
    diagonal = lax.broadcasted_iota(jnp.int32, (LANES, LANES), 0) == lax.broadcasted_iota(
        jnp.int32, (LANES, LANES), 1
    )

    def step(k, carry):
        for kk in range(blocks):

            @pl.when(k == kk)
            def _():
                here = kk * LANES
                columns = slice(here, here + LANES)
                left = packed[starts[kk] : starts[kk] + total - here, :] * (1.0 / total_rows)
                if kk:
                    left = left - dot_nt(lower[here:, :here], lower[columns, :here])
                corner[...] = left[:LANES] + jnp.where(diagonal, penalty, 0.0)
                if kk < blocks - 1:
                    lower[here + LANES : width, columns] = left[LANES : width - here]
                old = block_ref[
                    kk * BLOCK_ROWS + WEIGHT_ROW : kk * BLOCK_ROWS + WEIGHT_ROW + EXTRA, :
                ]
                lower[width:, columns] = left[width - here :] - penalty * old

        inverse_factor(corner, inverse.at[k])

        for kk in range(blocks):

            @pl.when(k == kk)
            def _():
                here = kk * LANES
                columns = slice(here, here + LANES)
                lower[here + LANES :, columns] = dot_nt(
                    lower[here + LANES :, columns], inverse[kk]
                )

        return carry

    lax.fori_loop(0, blocks, step, 0)
    for kk in reversed(range(blocks)):
        here = kk * LANES
        columns = slice(here, here + LANES)
        right = lower[width:, columns]
        if kk < blocks - 1:
            right = right - jnp.dot(
                change_ref[:, here + LANES :],
                lower[here + LANES : width, columns],
                precision=HIGHEST,
                preferred_element_type=F32,
            )
        change = jnp.dot(right, inverse[kk], precision=HIGHEST, preferred_element_type=F32)
        change_ref[:, columns] = change
        new_ref[:, columns] = change + block_ref[
            kk * BLOCK_ROWS + WEIGHT_ROW : kk * BLOCK_ROWS + WEIGHT_ROW + EXTRA, :
        ]


def solved(half, other, block, core, total_rows, width):
    out = jax.ShapeDtypeStruct((EXTRA, width), F32)
    return call(
        functools.partial(solve_kernel, total_rows),
        (out, out),
        core,
        half,
        other,
        block,
        scalars=1,
        scratch=(
            pltpu.VMEM((2 * HALF, LANES), F32),
            pltpu.VMEM((width + EXTRA, width), F32),
            pltpu.VMEM((width // LANES, LANES, LANES), F32),
            pltpu.VMEM((LANES, LANES), F32),
        ),
    )


def body(samples, residual, projections, phases, weights, block_order):
    outs = residual.shape[1]
    total_rows = samples.shape[0] * lax.axis_size(ROWS_FEAT)
    block = updated_block(projections, phases, weights, block_order[0])
    features, keep, send = products(samples, block, residual)
    half, other = total_of(keep, send)
    change, new = solved(
        half, other, block, index_of("core").reshape(1), total_rows, projections.shape[2]
    )
    residual = residual - dot_nt(features, change)[:, :outs]
    return residual, new[:outs].T[None]


def solution(mesh):
    finer = Mesh(mesh.devices.reshape(8, 4, 2, mesh.shape["feat"]), ROWS_FEAT)
    specs = (
        P(ROWS_FEAT, None),
        P(ROWS_FEAT, None),
        P("feat", None, None),
        P("feat", None),
        P("feat", None, None),
        P(),
    )
    return jax.shard_map(
        body, mesh=finer, in_specs=specs, out_specs=(P(ROWS_FEAT, None), P()), check_vma=False
    )
```

```python
import functools

import jax
import jax.numpy as jnp
from jax import lax
from jax.experimental import pallas as pl
from jax.experimental.pallas import tpu as pltpu
from jax.sharding import Mesh
from jax.sharding import PartitionSpec as P

ROWS = ("z", "x", "core")
ROWS_FEAT = ("z", "x", "core", "feat")
HIGHEST = lax.Precision.HIGHEST
F32 = jnp.float32

root_two = 1.4142135623730951
penalty = 0.05

LANES = 128
CHUNK = 80
PHASE_ROW = 440
WEIGHT_ROW = 448
BLOCK_ROWS = 640
EXTRA = 152
HALF = 3072

INTERPRET = False


def call(kernel, out_shape, *args, scalars=0, scratch=(), mib=12):
    specs = [pl.BlockSpec(memory_space=pltpu.SMEM)] * scalars
    specs += [pl.BlockSpec(memory_space=pltpu.VMEM)] * (len(args) - scalars)
    outs = jax.tree.map(lambda _: pl.BlockSpec(memory_space=pltpu.VMEM), out_shape)
    return pl.pallas_call(
        kernel,
        out_shape=out_shape,
        in_specs=specs,
        out_specs=outs,
        scratch_shapes=list(scratch),
        compiler_params=pltpu.CompilerParams(vmem_limit_bytes=mib * 2**20),
        interpret=INTERPRET,
    )(*args)


def rows_of(count):
    return jax.ShapeDtypeStruct((count, LANES), F32)


def shifted(x, axis, by):
    size = lax.axis_size(axis)
    return lax.ppermute(x, axis, [(i, (i + by) % size) for i in range(size)])


def from_others(pieces, axis):
    return [shifted(piece, axis, s) for s, piece in enumerate(pieces, 1)]


def to_others(piece, axis):
    return [shifted(piece, axis, s) for s in range(1, lax.axis_size(axis))]


def exchanged(x, axis):
    return lax.all_to_all(x, axis, split_axis=0, concat_axis=0, tiled=True)


def repeated(x, count):
    def kernel(x_ref, out_ref):
        rows = x_ref.shape[0]
        for s in range(count):
            out_ref[s * rows : (s + 1) * rows, :] = x_ref[...]

    return call(kernel, rows_of(count * x.shape[0]), x)


def wrapped(value, size):
    return lax.rem(value + size, size)


def index_of(axis):
    return lax.axis_index(axis).astype(jnp.int32)


def placed(me, piece, others):
    count, rows = len(others) + 1, piece.shape[0]

    def kernel(me_ref, *refs):
        out_ref = refs[-1]
        for s in range(count):
            at = wrapped(me_ref[0] - s, count)
            out_ref[pl.ds(pl.multiple_of(at * rows, 8), rows), :] = refs[s][...]

    return call(kernel, rows_of(count * rows), me.reshape(1), piece, *others, scalars=1)


def placed_pair(mes, pair, others):
    count, rows = len(others[0]) + 1, pair[0].shape[0]

    def kernel(me_ref, *refs):
        ins, outs = refs[:-2], refs[-2:]
        for c in range(2):
            for s in range(count):
                at = wrapped(me_ref[c] - s, count)
                outs[c][pl.ds(pl.multiple_of(at * rows, 8), rows), :] = ins[c * count + s][...]

    args = [x for own, rest in zip(pair, others) for x in (own, *rest)]
    return call(
        kernel, (rows_of(count * rows),) * 2, jnp.stack(mes), *args, scalars=1
    )


def dot_nt(a, b):
    return lax.dot_general(
        a, b, (((1,), (1,)), ((), ())), precision=HIGHEST, preferred_element_type=F32
    )


def chunk_of(projections, phases, weights, block_id):
    per_device = projections.shape[0]
    depth, width = projections.shape[1], projections.shape[2]
    outs = weights.shape[2]
    slot = block_id % per_device
    column = (index_of("core") * lax.axis_size("x") + index_of("x")) * LANES
    basis = lax.dynamic_slice(projections, (slot, 0, column), (1, depth, LANES))[0]
    phase = lax.dynamic_slice(phases, (slot, column), (1, LANES))
    old = lax.dynamic_slice(weights, (slot, column, 0), (1, LANES, outs))[0].T
    stacked = jnp.concatenate(
        [
            basis,
            phase,
            jnp.zeros((WEIGHT_ROW - depth - 1, LANES), F32),
            old,
            jnp.zeros((BLOCK_ROWS - WEIGHT_ROW - outs, LANES), F32),
        ]
    )
    return lax.dynamic_slice(stacked, (index_of("z") * CHUNK, 0), (CHUNK, LANES))


def updated_block(projections, phases, weights, block_id):
    per_device = projections.shape[0]
    chunk = chunk_of(projections, phases, weights, block_id)
    feat = index_of("feat")
    distance = wrapped(feat - block_id // per_device, lax.axis_size("feat"))
    chosen = chunk
    for s, other in enumerate(to_others(chunk, "feat"), 1):
        chosen = jnp.where(distance == s, other, chosen)
    part = exchanged(repeated(chosen, lax.axis_size("z")), "z")
    part = placed(index_of("x"), part, to_others(part, "x"))
    return placed(index_of("core"), part, to_others(part, "core"))


def cosine(x):
    turns = jnp.round(x * 0.15915494309189535)
    rest = (x - turns * 6.28125) - turns * 0.0019353071795864769
    sq = rest * rest * 0.25
    c = 2.08767569878681e-09
    for term in (
        -2.755731922398589e-07,
        2.48015873015873e-05,
        -0.001388888888888889,
        0.041666666666666664,
        -0.5,
        1.0,
    ):
        c = c * sq + term
    return 2.0 * (c * c) - 1.0


def products_kernel(core_ref, samples_ref, block_ref, residual_ref, features_ref, keep_ref, send_ref, points, turned, packed):
    blocks = features_ref.shape[0] // LANES
    depth, outs = samples_ref.shape[0], residual_ref.shape[0]
    width = blocks * LANES
    total = width + EXTRA
    points[:depth, :] = samples_ref[...]
    tail = (points.shape[0] - depth, points.shape[1])
    points[depth:, :] = jnp.where(lax.broadcasted_iota(jnp.int32, tail, 0) == PHASE_ROW - depth, 1.0, 0.0)
    for k in range(blocks):
        projected = lax.dot_general(
            block_ref[k * BLOCK_ROWS : k * BLOCK_ROWS + points.shape[0], :],
            points[...],
            (((0,), (0,)), ((), ())),
            precision=HIGHEST,
            preferred_element_type=F32,
        )
        features = root_two * cosine(projected)
        features_ref[k * LANES : (k + 1) * LANES, :] = features
        turned[k * LANES : (k + 1) * LANES, :] = features
    turned[width + EXTRA - 8 :, :] = jnp.zeros((8, turned.shape[1]), F32)
    turned[width : width + outs, :] = residual_ref[...]
    at = 0
    for k in range(blocks):
        count = total - k * LANES
        packed[at : at + count, :] = dot_nt(
            turned[k * LANES :, :], features_ref[k * LANES : (k + 1) * LANES, :]
        )
        at += count
    packed[at:, :] = jnp.zeros((packed.shape[0] - at, LANES), F32)
    mine = pl.multiple_of(core_ref[0] * HALF, 8)
    theirs = pl.multiple_of((1 - core_ref[0]) * HALF, 8)
    keep_ref[...] = packed[pl.ds(mine, HALF), :]
    send_ref[...] = packed[pl.ds(theirs, HALF), :]


def products(samples, block, residual):
    rows, width = samples.shape[1], block.shape[0] // BLOCK_ROWS * LANES
    return call(
        products_kernel,
        (jax.ShapeDtypeStruct((width, rows), F32), rows_of(HALF), rows_of(HALF)),
        index_of("core").reshape(1),
        samples,
        block,
        residual,
        scalars=1,
        scratch=(
            pltpu.VMEM((WEIGHT_ROW, rows), F32),
            pltpu.VMEM((width + EXTRA, rows), F32),
            pltpu.VMEM((2 * HALF, LANES), F32),
        ),
        mib=24,
    )


def summed_split(mes, groups, parts):
    joined = sum(group[0].shape[0] for group in groups)
    share = joined // len(mes)
    rows = share // parts
    sizes = [len(group) for group in groups]

    def kernel(me_ref, *refs):
        count = sum(sizes)
        ins, outs, scratch = refs[:count], refs[count:-1], refs[-1]
        first = at = 0
        for size in sizes:
            acc = ins[first][...]
            for ref in ins[first + 1 : first + size]:
                acc = acc + ref[...]
            scratch[at : at + acc.shape[0], :] = acc
            at += acc.shape[0]
            first += size
        for c in range(len(mes)):
            for s in range(parts):
                piece = wrapped(me_ref[c] + s, parts)
                start = pl.multiple_of(c * share + piece * rows, 8)
                outs[c * parts + s][...] = scratch[pl.ds(start, rows), :]

    outs = call(
        kernel,
        (rows_of(rows),) * (parts * len(mes)),
        jnp.stack(mes),
        *[x for group in groups for x in group],
        scalars=1,
        scratch=(pltpu.VMEM((joined, LANES), F32),),
    )
    return [outs[c * parts : (c + 1) * parts] for c in range(len(mes))]


def joined_sums(groups):
    sizes = [len(group) for group in groups]

    def kernel(*refs):
        first = at = 0
        for size in sizes:
            acc = refs[first][...]
            for ref in refs[first + 1 : first + size]:
                acc = acc + ref[...]
            refs[-1][at : at + acc.shape[0], :] = acc
            at += acc.shape[0]
            first += size

    joined = sum(group[0].shape[0] for group in groups)
    return call(kernel, rows_of(joined), *[x for group in groups for x in group])


def added_copies(x, count):
    rows = x.shape[0] // count

    def kernel(x_ref, out_ref):
        acc = x_ref[:rows, :]
        for s in range(1, count):
            acc = acc + x_ref[s * rows : (s + 1) * rows, :]
        for s in range(count):
            out_ref[s * rows : (s + 1) * rows, :] = acc

    return call(kernel, rows_of(x.shape[0]), x)


def total_of(keep, send):
    x, y = index_of("x"), index_of("feat")
    halves = [[keep, *from_others([send], "core")]]
    a, b = summed_split((x, y), halves, lax.axis_size("x"))
    a = [a[0], *from_others(a[1:], "x")]
    b = [b[0], *from_others(b[1:], "feat")]
    a, b = summed_split((y, x), (a, b), lax.axis_size("x"))
    a = [a[0], *from_others(a[1:], "feat")]
    b = [b[0], *from_others(b[1:], "x")]
    each = exchanged(joined_sums((a, b)), "z")
    both = exchanged(added_copies(each, lax.axis_size("z")), "z")
    a, b = both[: both.shape[0] // 2], both[both.shape[0] // 2 :]
    a, b = placed_pair((y, x), (a, b), (to_others(a, "feat"), to_others(b, "x")))
    a, b = placed_pair((x, y), (a, b), (to_others(a, "x"), to_others(b, "feat")))
    return a, b, shifted(a, "core", 1), shifted(b, "core", 1)


def across_sublanes(tile, row):
    return jnp.broadcast_to(tile[row : row + 1, :], tile.shape)


def columns_of(tile, first):
    return [jnp.broadcast_to(tile[:, first + q : first + q + 1], tile.shape) for q in range(8)]


def inverse_factor(source, target):
    tiles = LANES // 8
    lane = lax.broadcasted_iota(jnp.int32, (8, LANES), 1)
    sub = lax.broadcasted_iota(jnp.int32, (8, LANES), 0)
    rows = [source[8 * v : 8 * v + 8, :] for v in range(tiles)]
    ahead = columns_of(rows[0], 0)
    for b in range(tiles):
        inside = (lane >= 8 * b) & (lane < 8 * b + 8)
        columns = ahead
        tile = jnp.where(inside, jnp.where(lane == 8 * b + sub, 1.0, 0.0), rows[b])
        if b + 1 < tiles:
            ahead = columns_of(rows[b + 1], 8 * b + 8)
        pivots = jnp.ones((8, LANES), F32)
        inverses, multiples, tops = [], [], []
        for q in range(8):
            pivot = across_sublanes(columns[q], q)
            pivots = jnp.where(sub == q, pivot, pivots)
            inverse = 1.0 / pivot
            factor = jnp.where(sub > q, columns[q] * inverse, 0.0)
            multiple = {}
            for later in range(q + 1, 8):
                multiple[later] = across_sublanes(columns[later], q)
                columns[later] = columns[later] - factor * multiple[later]
            top = across_sublanes(tile, q)
            tile = tile - factor * top
            inverses.append(inverse)
            multiples.append(multiple)
            tops.append(top)
        target[8 * b : 8 * b + 8, :] = jnp.where(
            lane <= 8 * b + sub, tile * lax.rsqrt(pivots), 0.0
        )
        for v in range(b + 1, tiles):
            columns = columns_of(rows[v], 8 * b)
            below = jnp.where(inside, 0.0, rows[v])
            for q in range(8):
                factor = columns[q] * inverses[q]
                if v == b + 1:
                    for later in range(8):
                        ahead[later] = ahead[later] - factor * across_sublanes(columns[q], later)
                for later in range(q + 1, 8):
                    columns[later] = columns[later] - factor * multiples[q][later]
                below = below - factor * tops[q]
            rows[v] = below


def solve_kernel(
    total_rows, core_ref, *refs
):
    sums, refs = refs[:4], refs[4:]
    block_ref, features_ref, residual_ref, left_ref, new_ref = refs[:5]
    packed, lower, inverse, corner, change_ref = refs[5:]
    outs = residual_ref.shape[0]
    width = change_ref.shape[1]
    blocks = width // LANES
    total = width + EXTRA
    quarter = HALF // 2
    for n, ref in enumerate(sums):
        half = core_ref[0] if n < 2 else 1 - core_ref[0]
        packed[pl.ds(pl.multiple_of(half * HALF + n % 2 * quarter, 8), quarter), :] = ref[...]
    starts = [k * total - LANES * (k * (k - 1) // 2) for k in range(blocks)]
    diagonal = lax.broadcasted_iota(jnp.int32, (LANES, LANES), 0) == lax.broadcasted_iota(
        jnp.int32, (LANES, LANES), 1
    )

    def step(k, carry):
        for kk in range(blocks):

            @pl.when(k == kk)
            def _():
                here = kk * LANES
                columns = slice(here, here + LANES)
                left = packed[starts[kk] : starts[kk] + total - here, :] * (1.0 / total_rows)
                if kk:
                    left = left - dot_nt(lower[here:, :here], lower[columns, :here])
                corner[...] = left[:LANES] + jnp.where(diagonal, penalty, 0.0)
                if kk < blocks - 1:
                    lower[here + LANES : width, columns] = left[LANES : width - here]
                old = block_ref[
                    kk * BLOCK_ROWS + WEIGHT_ROW : kk * BLOCK_ROWS + WEIGHT_ROW + EXTRA, :
                ]
                lower[width:, columns] = left[width - here :] - penalty * old

        inverse_factor(corner, inverse.at[k])

        for kk in range(blocks):

            @pl.when(k == kk)
            def _():
                here = kk * LANES
                columns = slice(here, here + LANES)
                lower[here + LANES :, columns] = dot_nt(
                    lower[here + LANES :, columns], inverse[kk]
                )

        return carry

    lax.fori_loop(0, blocks, step, 0)
    for kk in reversed(range(blocks)):
        here = kk * LANES
        columns = slice(here, here + LANES)
        right = lower[width:, columns]
        if kk < blocks - 1:
            right = right - jnp.dot(
                change_ref[:, here + LANES :],
                lower[here + LANES : width, columns],
                precision=HIGHEST,
                preferred_element_type=F32,
            )
        change = jnp.dot(right, inverse[kk], precision=HIGHEST, preferred_element_type=F32)
        change_ref[:, columns] = change
        old = block_ref[kk * BLOCK_ROWS + WEIGHT_ROW : kk * BLOCK_ROWS + WEIGHT_ROW + outs, :]
        new_ref[:, 0, columns] = change[:outs] + old
    left_ref[...] = residual_ref[...] - jnp.dot(
        change_ref[...], features_ref[...], precision=HIGHEST, preferred_element_type=F32
    )[:outs]


def solved(sums, block, features, residual, core, total_rows):
    width, rows = features.shape
    outs = residual.shape[0]
    return call(
        functools.partial(solve_kernel, total_rows),
        (
            jax.ShapeDtypeStruct((outs, rows), F32),
            jax.ShapeDtypeStruct((outs, 1, width), F32),
        ),
        core,
        *sums,
        block,
        features,
        residual,
        scalars=1,
        scratch=(
            pltpu.VMEM((2 * HALF, LANES), F32),
            pltpu.VMEM((width + EXTRA, width), F32),
            pltpu.VMEM((width // LANES, LANES, LANES), F32),
            pltpu.VMEM((LANES, LANES), F32),
            pltpu.VMEM((EXTRA, width), F32),
        ),
        mib=40,
    )


def body(samples, residual, projections, phases, weights, block_order):
    total_rows = samples.shape[0] * lax.axis_size(ROWS_FEAT)
    residual = residual.T
    block = updated_block(projections, phases, weights, block_order[0])
    features, keep, send = products(samples.T, block, residual)
    sums = total_of(keep, send)
    left, new = solved(
        sums, block, features, residual, index_of("core").reshape(1), total_rows
    )
    return left.T, jnp.transpose(new, (1, 2, 0))


def solution(mesh):
    finer = Mesh(mesh.devices.reshape(8, 4, 2, mesh.shape["feat"]), ROWS_FEAT)
    specs = (
        P(ROWS_FEAT, None),
        P(ROWS_FEAT, None),
        P("feat", None, None),
        P("feat", None),
        P("feat", None, None),
        P(),
    )
    return jax.shard_map(
        body, mesh=finer, in_specs=specs, out_specs=(P(ROWS_FEAT, None), P()), check_vma=False
    )
```

```python
import functools

import jax
import jax.numpy as jnp
from jax import lax
from jax.experimental import pallas as pl
from jax.experimental.pallas import tpu as pltpu
from jax.sharding import Mesh
from jax.sharding import PartitionSpec as P

ROWS = ("z", "x", "core")
ROWS_FEAT = ("z", "x", "core", "feat")
HIGHEST = lax.Precision.HIGHEST
F32 = jnp.float32

root_two = 1.4142135623730951
penalty = 0.05

LANES = 128
CHUNK = 20
PHASE_ROW = 440
WEIGHT_ROW = 448
BLOCK_ROWS = 640
EXTRA = 152
HALF = 3072

INTERPRET = False


def call(kernel, out_shape, *args, scalars=0, scratch=(), mib=12):
    specs = [pl.BlockSpec(memory_space=pltpu.SMEM)] * scalars
    specs += [pl.BlockSpec(memory_space=pltpu.VMEM)] * (len(args) - scalars)
    outs = jax.tree.map(lambda _: pl.BlockSpec(memory_space=pltpu.VMEM), out_shape)
    return pl.pallas_call(
        kernel,
        out_shape=out_shape,
        in_specs=specs,
        out_specs=outs,
        scratch_shapes=list(scratch),
        compiler_params=pltpu.CompilerParams(vmem_limit_bytes=mib * 2**20),
        interpret=INTERPRET,
    )(*args)


def rows_of(count):
    return jax.ShapeDtypeStruct((count, LANES), F32)


def shifted(x, axis, by):
    size = lax.axis_size(axis)
    return lax.ppermute(x, axis, [(i, (i + by) % size) for i in range(size)])


PLANE = ("x", "feat")


def exchanged(x, axis):
    return lax.all_to_all(x, axis, split_axis=0, concat_axis=0, tiled=True)


def repeated(x, count):
    def kernel(x_ref, out_ref):
        rows = x_ref.shape[0]
        for s in range(count):
            out_ref[s * rows : (s + 1) * rows, :] = x_ref[...]

    return call(kernel, rows_of(count * x.shape[0]), x)


def index_of(axis):
    return lax.axis_index(axis).astype(jnp.int32)


def placed(me, piece, other):
    rows = piece.shape[0]

    def kernel(me_ref, piece_ref, other_ref, out_ref):
        out_ref[pl.ds(pl.multiple_of(me_ref[0] * rows, 8), rows), :] = piece_ref[...]
        out_ref[pl.ds(pl.multiple_of((1 - me_ref[0]) * rows, 8), rows), :] = other_ref[...]

    return call(kernel, rows_of(2 * rows), me.reshape(1), piece, other, scalars=1)


def dot_nt(a, b):
    return lax.dot_general(
        a, b, (((1,), (1,)), ((), ())), precision=HIGHEST, preferred_element_type=F32
    )


def chunks_of(projections, phases, weights, block_id):
    per_device = projections.shape[0]
    depth, width = projections.shape[1], projections.shape[2]
    outs = weights.shape[2]
    slot = block_id % per_device
    column = (index_of("core") * lax.axis_size("x") + index_of("x")) * LANES
    basis = lax.dynamic_slice(projections, (slot, 0, column), (1, depth, LANES))[0]
    phase = lax.dynamic_slice(phases, (slot, column), (1, LANES))
    old = lax.dynamic_slice(weights, (slot, column, 0), (1, LANES, outs))[0].T
    stacked = jnp.concatenate(
        [
            basis,
            phase,
            jnp.zeros((WEIGHT_ROW - depth - 1, LANES), F32),
            old,
            jnp.zeros((BLOCK_ROWS - WEIGHT_ROW - outs, LANES), F32),
        ]
    )
    size = lax.axis_size("feat")
    return lax.dynamic_slice(
        stacked.reshape(size, BLOCK_ROWS // size, LANES),
        (0, index_of("z") * CHUNK, 0),
        (size, CHUNK, LANES),
    )


def updated_block(projections, phases, weights, block_id):
    pieces = exchanged(chunks_of(projections, phases, weights, block_id), "feat")
    chosen = lax.dynamic_index_in_dim(pieces, block_id // projections.shape[0], 0, True)
    copies = jnp.broadcast_to(chosen, (lax.axis_size("z"), CHUNK, LANES))
    part = exchanged(copies, "z").reshape(-1, LANES)
    part = exchanged(repeated(part, lax.axis_size(PLANE)), PLANE)
    return placed(index_of("core"), part, shifted(part, "core", 1))


def cosine(x):
    turns = jnp.round(x * 0.15915494309189535)
    rest = (x - turns * 6.28125) - turns * 0.0019353071795864769
    sq = rest * rest * 0.25
    c = 2.08767569878681e-09
    for term in (
        -2.755731922398589e-07,
        2.48015873015873e-05,
        -0.001388888888888889,
        0.041666666666666664,
        -0.5,
        1.0,
    ):
        c = c * sq + term
    return 2.0 * (c * c) - 1.0


def products_kernel(core_ref, samples_ref, block_ref, residual_ref, features_ref, keep_ref, send_ref, points, turned, packed):
    blocks = features_ref.shape[0] // LANES
    depth, outs = samples_ref.shape[0], residual_ref.shape[0]
    width = blocks * LANES
    total = width + EXTRA
    points[:depth, :] = samples_ref[...]
    tail = (points.shape[0] - depth, points.shape[1])
    points[depth:, :] = jnp.where(lax.broadcasted_iota(jnp.int32, tail, 0) == PHASE_ROW - depth, 1.0, 0.0)
    for k in range(blocks):
        projected = lax.dot_general(
            block_ref[k * BLOCK_ROWS : k * BLOCK_ROWS + points.shape[0], :],
            points[...],
            (((0,), (0,)), ((), ())),
            precision=HIGHEST,
            preferred_element_type=F32,
        )
        features = root_two * cosine(projected)
        features_ref[k * LANES : (k + 1) * LANES, :] = features
        turned[k * LANES : (k + 1) * LANES, :] = features
    turned[width + EXTRA - 8 :, :] = jnp.zeros((8, turned.shape[1]), F32)
    turned[width : width + outs, :] = residual_ref[...]
    at = 0
    for k in range(blocks):
        count = total - k * LANES
        packed[at : at + count, :] = dot_nt(
            turned[k * LANES :, :], features_ref[k * LANES : (k + 1) * LANES, :]
        )
        at += count
    packed[at:, :] = jnp.zeros((packed.shape[0] - at, LANES), F32)
    mine = pl.multiple_of(core_ref[0] * HALF, 8)
    theirs = pl.multiple_of((1 - core_ref[0]) * HALF, 8)
    keep_ref[...] = packed[pl.ds(mine, HALF), :]
    send_ref[...] = packed[pl.ds(theirs, HALF), :]


def products(samples, block, residual):
    rows, width = samples.shape[1], block.shape[0] // BLOCK_ROWS * LANES
    return call(
        products_kernel,
        (jax.ShapeDtypeStruct((width, rows), F32), rows_of(HALF), rows_of(HALF)),
        index_of("core").reshape(1),
        samples,
        block,
        residual,
        scalars=1,
        scratch=(
            pltpu.VMEM((WEIGHT_ROW, rows), F32),
            pltpu.VMEM((width + EXTRA, rows), F32),
            pltpu.VMEM((2 * HALF, LANES), F32),
        ),
        mib=24,
    )


def added(a, b):
    def kernel(a_ref, b_ref, out_ref):
        out_ref[...] = a_ref[...] + b_ref[...]

    return call(kernel, rows_of(a.shape[0]), a, b)


def added_parts(x, count):
    rows = x.shape[0] // count

    def kernel(x_ref, out_ref):
        acc = x_ref[:rows, :]
        for s in range(1, count):
            acc = acc + x_ref[s * rows : (s + 1) * rows, :]
        out_ref[...] = acc

    return call(kernel, rows_of(rows), x)


def added_copies(x, count):
    rows = x.shape[0] // count

    def kernel(x_ref, out_ref):
        acc = x_ref[:rows, :]
        for s in range(1, count):
            acc = acc + x_ref[s * rows : (s + 1) * rows, :]
        for s in range(count):
            out_ref[s * rows : (s + 1) * rows, :] = acc

    return call(kernel, rows_of(x.shape[0]), x)


def total_of(keep, send):
    plane, line = lax.axis_size(PLANE), lax.axis_size("z")
    half = added(keep, shifted(send, "core", 1))
    part = added_parts(exchanged(half, PLANE), plane)
    part = exchanged(added_copies(exchanged(part, "z"), line), "z")
    half = exchanged(repeated(part, plane), PLANE)
    return half, shifted(half, "core", 1)


def across_sublanes(tile, row):
    return jnp.broadcast_to(tile[row : row + 1, :], tile.shape)


def columns_of(tile, first):
    return [jnp.broadcast_to(tile[:, first + q : first + q + 1], tile.shape) for q in range(8)]


def inverse_factor(source, target):
    tiles = LANES // 8
    lane = lax.broadcasted_iota(jnp.int32, (8, LANES), 1)
    sub = lax.broadcasted_iota(jnp.int32, (8, LANES), 0)
    rows = [source[8 * v : 8 * v + 8, :] for v in range(tiles)]
    ahead = columns_of(rows[0], 0)
    for b in range(tiles):
        inside = (lane >= 8 * b) & (lane < 8 * b + 8)
        columns = ahead
        tile = jnp.where(inside, jnp.where(lane == 8 * b + sub, 1.0, 0.0), rows[b])
        if b + 1 < tiles:
            ahead = columns_of(rows[b + 1], 8 * b + 8)
        pivots = jnp.ones((8, LANES), F32)
        inverses, multiples, tops = [], [], []
        for q in range(8):
            pivot = across_sublanes(columns[q], q)
            pivots = jnp.where(sub == q, pivot, pivots)
            inverse = 1.0 / pivot
            factor = jnp.where(sub > q, columns[q] * inverse, 0.0)
            multiple = {}
            for later in range(q + 1, 8):
                multiple[later] = across_sublanes(columns[later], q)
                columns[later] = columns[later] - factor * multiple[later]
            top = across_sublanes(tile, q)
            tile = tile - factor * top
            inverses.append(inverse)
            multiples.append(multiple)
            tops.append(top)
        target[8 * b : 8 * b + 8, :] = jnp.where(
            lane <= 8 * b + sub, tile * lax.rsqrt(pivots), 0.0
        )
        for v in range(b + 1, tiles):
            columns = columns_of(rows[v], 8 * b)
            below = jnp.where(inside, 0.0, rows[v])
            for q in range(8):
                factor = columns[q] * inverses[q]
                if v == b + 1:
                    for later in range(8):
                        ahead[later] = ahead[later] - factor * across_sublanes(columns[q], later)
                for later in range(q + 1, 8):
                    columns[later] = columns[later] - factor * multiples[q][later]
                below = below - factor * tops[q]
            rows[v] = below


def solve_kernel(
    total_rows, core_ref, *refs
):
    sums, refs = refs[:2], refs[2:]
    block_ref, features_ref, residual_ref, left_ref, new_ref = refs[:5]
    packed, lower, inverse, corner, change_ref = refs[5:]
    outs = residual_ref.shape[0]
    width = change_ref.shape[1]
    blocks = width // LANES
    total = width + EXTRA
    for half, ref in zip((core_ref[0], 1 - core_ref[0]), sums):
        packed[pl.ds(pl.multiple_of(half * HALF, 8), HALF), :] = ref[...]
    starts = [k * total - LANES * (k * (k - 1) // 2) for k in range(blocks)]
    diagonal = lax.broadcasted_iota(jnp.int32, (LANES, LANES), 0) == lax.broadcasted_iota(
        jnp.int32, (LANES, LANES), 1
    )

    def step(k, carry):
        for kk in range(blocks):

            @pl.when(k == kk)
            def _():
                here = kk * LANES
                columns = slice(here, here + LANES)
                left = packed[starts[kk] : starts[kk] + total - here, :] * (1.0 / total_rows)
                if kk:
                    left = left - dot_nt(lower[here:, :here], lower[columns, :here])
                corner[...] = left[:LANES] + jnp.where(diagonal, penalty, 0.0)
                if kk < blocks - 1:
                    lower[here + LANES : width, columns] = left[LANES : width - here]
                old = block_ref[
                    kk * BLOCK_ROWS + WEIGHT_ROW : kk * BLOCK_ROWS + WEIGHT_ROW + EXTRA, :
                ]
                lower[width:, columns] = left[width - here :] - penalty * old

        inverse_factor(corner, inverse.at[k])

        for kk in range(blocks):

            @pl.when(k == kk)
            def _():
                here = kk * LANES
                columns = slice(here, here + LANES)
                lower[here + LANES :, columns] = dot_nt(
                    lower[here + LANES :, columns], inverse[kk]
                )

        return carry

    lax.fori_loop(0, blocks, step, 0)
    for kk in reversed(range(blocks)):
        here = kk * LANES
        columns = slice(here, here + LANES)
        right = lower[width:, columns]
        if kk < blocks - 1:
            right = right - jnp.dot(
                change_ref[:, here + LANES :],
                lower[here + LANES : width, columns],
                precision=HIGHEST,
                preferred_element_type=F32,
            )
        change = jnp.dot(right, inverse[kk], precision=HIGHEST, preferred_element_type=F32)
        change_ref[:, columns] = change
        old = block_ref[kk * BLOCK_ROWS + WEIGHT_ROW : kk * BLOCK_ROWS + WEIGHT_ROW + outs, :]
        new_ref[:, 0, columns] = change[:outs] + old
    left_ref[...] = residual_ref[...] - jnp.dot(
        change_ref[...], features_ref[...], precision=HIGHEST, preferred_element_type=F32
    )[:outs]


def solved(sums, block, features, residual, core, total_rows):
    width, rows = features.shape
    outs = residual.shape[0]
    return call(
        functools.partial(solve_kernel, total_rows),
        (
            jax.ShapeDtypeStruct((outs, rows), F32),
            jax.ShapeDtypeStruct((outs, 1, width), F32),
        ),
        core,
        *sums,
        block,
        features,
        residual,
        scalars=1,
        scratch=(
            pltpu.VMEM((2 * HALF, LANES), F32),
            pltpu.VMEM((width + EXTRA, width), F32),
            pltpu.VMEM((width // LANES, LANES, LANES), F32),
            pltpu.VMEM((LANES, LANES), F32),
            pltpu.VMEM((EXTRA, width), F32),
        ),
        mib=40,
    )


def body(samples, residual, projections, phases, weights, block_order):
    total_rows = samples.shape[0] * lax.axis_size(ROWS_FEAT)
    residual = residual.T
    block = updated_block(projections, phases, weights, block_order[0])
    features, keep, send = products(samples.T, block, residual)
    sums = total_of(keep, send)
    left, new = solved(
        sums, block, features, residual, index_of("core").reshape(1), total_rows
    )
    return left.T, jnp.transpose(new, (1, 2, 0))


def solution(mesh):
    finer = Mesh(mesh.devices.reshape(8, 4, 2, mesh.shape["feat"]), ROWS_FEAT)
    specs = (
        P(ROWS_FEAT, None),
        P(ROWS_FEAT, None),
        P("feat", None, None),
        P("feat", None),
        P("feat", None, None),
        P(),
    )
    return jax.shard_map(
        body, mesh=finer, in_specs=specs, out_specs=(P(ROWS_FEAT, None), P()), check_vma=False
    )
```

```python
import functools

import jax
import jax.numpy as jnp
from jax import lax
from jax.experimental import pallas as pl
from jax.experimental.pallas import tpu as pltpu
from jax.sharding import Mesh
from jax.sharding import PartitionSpec as P

ROWS = ("z", "x", "core")
ROWS_FEAT = ("z", "x", "core", "feat")
HIGHEST = lax.Precision.HIGHEST
F32 = jnp.float32
BF16 = jnp.bfloat16

root_two = 1.4142135623730951
penalty = 0.05

LANES = 128
CHUNK = 20
PHASE_ROW = 440
WEIGHT_ROW = 448
BLOCK_ROWS = 640
EXTRA = 152
HALF = 3072

INTERPRET = False


def call(kernel, out_shape, *args, scalars=0, scratch=(), mib=12):
    specs = [pl.BlockSpec(memory_space=pltpu.SMEM)] * scalars
    specs += [pl.BlockSpec(memory_space=pltpu.VMEM)] * (len(args) - scalars)
    outs = jax.tree.map(lambda _: pl.BlockSpec(memory_space=pltpu.VMEM), out_shape)
    return pl.pallas_call(
        kernel,
        out_shape=out_shape,
        in_specs=specs,
        out_specs=outs,
        scratch_shapes=list(scratch),
        compiler_params=pltpu.CompilerParams(vmem_limit_bytes=mib * 2**20),
        interpret=INTERPRET,
    )(*args)


def rows_of(count):
    return jax.ShapeDtypeStruct((count, LANES), F32)


def shifted(x, axis, by):
    size = lax.axis_size(axis)
    return lax.ppermute(x, axis, [(i, (i + by) % size) for i in range(size)])


PLANE = ("x", "feat")


def exchanged(x, axis):
    return lax.all_to_all(x, axis, split_axis=0, concat_axis=0, tiled=True)


def repeated(x, count):
    def kernel(x_ref, out_ref):
        rows = x_ref.shape[0]
        for s in range(count):
            out_ref[s * rows : (s + 1) * rows, :] = x_ref[...]

    return call(kernel, rows_of(count * x.shape[0]), x)


def index_of(axis):
    return lax.axis_index(axis).astype(jnp.int32)


def placed(me, piece, other):
    rows = piece.shape[0]

    def kernel(me_ref, piece_ref, other_ref, out_ref):
        out_ref[pl.ds(pl.multiple_of(me_ref[0] * rows, 8), rows), :] = piece_ref[...]
        out_ref[pl.ds(pl.multiple_of((1 - me_ref[0]) * rows, 8), rows), :] = other_ref[...]

    return call(kernel, rows_of(2 * rows), me.reshape(1), piece, other, scalars=1)


def split(x):
    high = x.astype(BF16)
    rest = x - high.astype(F32)
    middle = rest.astype(BF16)
    return high, middle, (rest - middle.astype(F32)).astype(BF16)


def dot_split(a, b, dim_a, dim_b):
    return lax.dot_general(
        jnp.concatenate([a[n] for n in (2, 0, 1, 1, 0, 0)], axis=dim_a),
        jnp.concatenate([b[n] for n in (0, 2, 1, 0, 1, 0)], axis=dim_b),
        (((dim_a,), (dim_b,)), ((), ())),
        preferred_element_type=F32,
    )


def chunks_of(projections, phases, weights, block_id):
    per_device = projections.shape[0]
    depth, width = projections.shape[1], projections.shape[2]
    outs = weights.shape[2]
    slot = block_id % per_device
    column = (index_of("core") * lax.axis_size("x") + index_of("x")) * LANES
    basis = lax.dynamic_slice(projections, (slot, 0, column), (1, depth, LANES))[0]
    phase = lax.dynamic_slice(phases, (slot, column), (1, LANES))
    old = lax.dynamic_slice(weights, (slot, column, 0), (1, LANES, outs))[0].T
    stacked = jnp.concatenate(
        [
            basis,
            phase,
            jnp.zeros((WEIGHT_ROW - depth - 1, LANES), F32),
            old,
            jnp.zeros((BLOCK_ROWS - WEIGHT_ROW - outs, LANES), F32),
        ]
    )
    size = lax.axis_size("feat")
    return lax.dynamic_slice(
        stacked.reshape(size, BLOCK_ROWS // size, LANES),
        (0, index_of("z") * CHUNK, 0),
        (size, CHUNK, LANES),
    )


def updated_block(projections, phases, weights, block_id):
    pieces = exchanged(chunks_of(projections, phases, weights, block_id), "feat")
    chosen = lax.dynamic_index_in_dim(pieces, block_id // projections.shape[0], 0, True)
    copies = jnp.broadcast_to(chosen, (lax.axis_size("z"), CHUNK, LANES))
    part = exchanged(copies, "z").reshape(-1, LANES)
    part = exchanged(repeated(part, lax.axis_size(PLANE)), PLANE)
    return placed(index_of("core"), part, shifted(part, "core", 1))


def cosine(x):
    turns = jnp.round(x * 0.15915494309189535)
    rest = (x - turns * 6.28125) - turns * 0.0019353071795864769
    sq = rest * rest * 0.25
    c = 2.08767569878681e-09
    for term in (
        -2.755731922398589e-07,
        2.48015873015873e-05,
        -0.001388888888888889,
        0.041666666666666664,
        -0.5,
        1.0,
    ):
        c = c * sq + term
    return 2.0 * (c * c) - 1.0


def products_kernel(core_ref, samples_ref, block_ref, residual_ref, features_ref, keep_ref, send_ref, points, extra, turned, packed):
    blocks = features_ref.shape[0] // LANES
    depth, outs = samples_ref.shape[0], residual_ref.shape[0]
    width = blocks * LANES
    total = width + EXTRA
    points[:depth, :] = samples_ref[...]
    tail = (points.shape[0] - depth, points.shape[1])
    points[depth:, :] = jnp.where(lax.broadcasted_iota(jnp.int32, tail, 0) == PHASE_ROW - depth, 1.0, 0.0)
    for k in range(blocks):
        projected = lax.dot_general(
            block_ref[k * BLOCK_ROWS : k * BLOCK_ROWS + points.shape[0], :],
            points[...],
            (((0,), (0,)), ((), ())),
            precision=HIGHEST,
            preferred_element_type=F32,
        )
        features = root_two * cosine(projected)
        features_ref[k * LANES : (k + 1) * LANES, :] = features
        for n, part in enumerate(split(features)):
            turned[n, k * LANES : (k + 1) * LANES, :] = part
    extra[EXTRA - 8 :, :] = jnp.zeros((8, extra.shape[1]), F32)
    extra[:outs, :] = residual_ref[...]
    for n, part in enumerate(split(extra[...])):
        turned[n, width : width + EXTRA, :] = part
    at = 0
    for k in range(blocks):
        count = total - k * LANES
        packed[at : at + count, :] = dot_split(
            [turned[n, k * LANES : total, :] for n in range(3)],
            [turned[n, k * LANES : (k + 1) * LANES, :] for n in range(3)],
            1,
            1,
        )
        at += count
    packed[at:, :] = jnp.zeros((packed.shape[0] - at, LANES), F32)
    mine = pl.multiple_of(core_ref[0] * HALF, 8)
    theirs = pl.multiple_of((1 - core_ref[0]) * HALF, 8)
    keep_ref[...] = packed[pl.ds(mine, HALF), :]
    send_ref[...] = packed[pl.ds(theirs, HALF), :]


def products(samples, block, residual):
    rows, width = samples.shape[1], block.shape[0] // BLOCK_ROWS * LANES
    return call(
        products_kernel,
        (jax.ShapeDtypeStruct((width, rows), F32), rows_of(HALF), rows_of(HALF)),
        index_of("core").reshape(1),
        samples,
        block,
        residual,
        scalars=1,
        scratch=(
            pltpu.VMEM((WEIGHT_ROW, rows), F32),
            pltpu.VMEM((EXTRA, rows), F32),
            pltpu.VMEM((3, width + EXTRA + 8, rows), BF16),
            pltpu.VMEM((2 * HALF, LANES), F32),
        ),
        mib=24,
    )


def added(a, b):
    def kernel(a_ref, b_ref, out_ref):
        out_ref[...] = a_ref[...] + b_ref[...]

    return call(kernel, rows_of(a.shape[0]), a, b)


def added_parts(x, count):
    rows = x.shape[0] // count

    def kernel(x_ref, out_ref):
        acc = x_ref[:rows, :]
        for s in range(1, count):
            acc = acc + x_ref[s * rows : (s + 1) * rows, :]
        out_ref[...] = acc

    return call(kernel, rows_of(rows), x)


def added_copies(x, count):
    rows = x.shape[0] // count

    def kernel(x_ref, out_ref):
        acc = x_ref[:rows, :]
        for s in range(1, count):
            acc = acc + x_ref[s * rows : (s + 1) * rows, :]
        for s in range(count):
            out_ref[s * rows : (s + 1) * rows, :] = acc

    return call(kernel, rows_of(x.shape[0]), x)


def total_of(keep, send):
    plane, line = lax.axis_size(PLANE), lax.axis_size("z")
    half = added(keep, shifted(send, "core", 1))
    part = added_parts(exchanged(half, PLANE), plane)
    part = exchanged(added_copies(exchanged(part, "z"), line), "z")
    half = exchanged(repeated(part, plane), PLANE)
    return half, shifted(half, "core", 1)


def across_sublanes(tile, row):
    return jnp.broadcast_to(tile[row : row + 1, :], tile.shape)


def columns_of(tile, first):
    return [jnp.broadcast_to(tile[:, first + q : first + q + 1], tile.shape) for q in range(8)]


def inverse_factor(source, target):
    tiles = LANES // 8
    lane = lax.broadcasted_iota(jnp.int32, (8, LANES), 1)
    sub = lax.broadcasted_iota(jnp.int32, (8, LANES), 0)
    rows = [source[8 * v : 8 * v + 8, :] for v in range(tiles)]
    ahead = columns_of(rows[0], 0)
    for b in range(tiles):
        inside = (lane >= 8 * b) & (lane < 8 * b + 8)
        columns = ahead
        tile = jnp.where(inside, jnp.where(lane == 8 * b + sub, 1.0, 0.0), rows[b])
        if b + 1 < tiles:
            ahead = columns_of(rows[b + 1], 8 * b + 8)
        pivots = jnp.ones((8, LANES), F32)
        inverses, multiples, tops = [], [], []
        for q in range(8):
            pivot = across_sublanes(columns[q], q)
            pivots = jnp.where(sub == q, pivot, pivots)
            inverse = 1.0 / pivot
            factor = jnp.where(sub > q, columns[q] * inverse, 0.0)
            multiple = {}
            for later in range(q + 1, 8):
                multiple[later] = across_sublanes(columns[later], q)
                columns[later] = columns[later] - factor * multiple[later]
            top = across_sublanes(tile, q)
            tile = tile - factor * top
            inverses.append(inverse)
            multiples.append(multiple)
            tops.append(top)
        target[8 * b : 8 * b + 8, :] = jnp.where(
            lane <= 8 * b + sub, tile * lax.rsqrt(pivots), 0.0
        )
        for v in range(b + 1, tiles):
            columns = columns_of(rows[v], 8 * b)
            below = jnp.where(inside, 0.0, rows[v])
            for q in range(8):
                factor = columns[q] * inverses[q]
                if v == b + 1:
                    for later in range(8):
                        ahead[later] = ahead[later] - factor * across_sublanes(columns[q], later)
                for later in range(q + 1, 8):
                    columns[later] = columns[later] - factor * multiples[q][later]
                below = below - factor * tops[q]
            rows[v] = below


def solve_kernel(
    total_rows, core_ref, *refs
):
    sums, refs = refs[:2], refs[2:]
    block_ref, features_ref, residual_ref, left_ref, new_ref = refs[:5]
    packed, lower, inverse, corner, raw, right_ref, change_ref = refs[5:]
    outs, rows = residual_ref.shape
    width = features_ref.shape[0]
    blocks = width // LANES
    total = width + EXTRA

    def parts(ref, rows, columns):
        return [ref[n, rows, columns] for n in range(3)]

    for half, ref in zip((core_ref[0], 1 - core_ref[0]), sums):
        packed[pl.ds(pl.multiple_of(half * HALF, 8), HALF), :] = ref[...]
    starts = [k * total - LANES * (k * (k - 1) // 2) for k in range(blocks)]
    diagonal = lax.broadcasted_iota(jnp.int32, (LANES, LANES), 0) == lax.broadcasted_iota(
        jnp.int32, (LANES, LANES), 1
    )

    def step(k, carry):
        for kk in range(blocks):

            @pl.when(k == kk)
            def _():
                here = kk * LANES
                columns = slice(here, here + LANES)
                left = packed[starts[kk] : starts[kk] + total - here, :] * (1.0 / total_rows)
                if kk:
                    left = left - dot_split(
                        parts(lower, slice(here, total), slice(0, here)),
                        parts(lower, columns, slice(0, here)),
                        1,
                        1,
                    )
                corner[...] = left[:LANES] + jnp.where(diagonal, penalty, 0.0)
                if kk < blocks - 1:
                    raw[here + LANES : width, :] = left[LANES : width - here]
                old = block_ref[
                    kk * BLOCK_ROWS + WEIGHT_ROW : kk * BLOCK_ROWS + WEIGHT_ROW + EXTRA, :
                ]
                raw[width:, :] = left[width - here :] - penalty * old

        inverse_factor(corner, inverse.at[k])

        for kk in range(blocks):

            @pl.when(k == kk)
            def _():
                here = kk * LANES
                columns = slice(here, here + LANES)
                below = dot_split(split(raw[here + LANES :, :]), split(inverse[kk]), 1, 1)
                right_ref[:, columns] = below[width - here - LANES :]
                for n, part in enumerate(split(below)):
                    lower[n, here + LANES : total, columns] = part

        return carry

    lax.fori_loop(0, blocks, step, 0)
    for kk in reversed(range(blocks)):
        here = kk * LANES
        columns = slice(here, here + LANES)
        right = right_ref[:, columns]
        if kk < blocks - 1:
            later = slice(here + LANES, width)
            right = right - dot_split(
                parts(change_ref, slice(0, EXTRA), later), parts(lower, later, columns), 1, 0
            )
        change = dot_split(split(right), split(inverse[kk]), 1, 0)
        for n, part in enumerate(split(change)):
            change_ref[n, :EXTRA, columns] = part
        old = block_ref[kk * BLOCK_ROWS + WEIGHT_ROW : kk * BLOCK_ROWS + WEIGHT_ROW + outs, :]
        new_ref[:, 0, columns] = change[:outs] + old
    left_ref[...] = residual_ref[...] - dot_split(
        parts(change_ref, slice(0, EXTRA), slice(0, width)), split(features_ref[...]), 1, 0
    )[:outs]


def solved(sums, block, features, residual, core, total_rows):
    width, rows = features.shape
    outs = residual.shape[0]
    return call(
        functools.partial(solve_kernel, total_rows),
        (
            jax.ShapeDtypeStruct((outs, rows), F32),
            jax.ShapeDtypeStruct((outs, 1, width), F32),
        ),
        core,
        *sums,
        block,
        features,
        residual,
        scalars=1,
        scratch=(
            pltpu.VMEM((2 * HALF, LANES), F32),
            pltpu.VMEM((3, width + EXTRA + 8, width), BF16),
            pltpu.VMEM((width // LANES, LANES, LANES), F32),
            pltpu.VMEM((LANES, LANES), F32),
            pltpu.VMEM((width + EXTRA, LANES), F32),
            pltpu.VMEM((EXTRA, width), F32),
            pltpu.VMEM((3, EXTRA + 8, width), BF16),
        ),
        mib=40,
    )


def body(samples, residual, projections, phases, weights, block_order):
    total_rows = samples.shape[0] * lax.axis_size(ROWS_FEAT)
    residual = residual.T
    block = updated_block(projections, phases, weights, block_order[0])
    features, keep, send = products(samples.T, block, residual)
    sums = total_of(keep, send)
    left, new = solved(
        sums, block, features, residual, index_of("core").reshape(1), total_rows
    )
    return left.T, jnp.transpose(new, (1, 2, 0))


def solution(mesh):
    finer = Mesh(mesh.devices.reshape(8, 4, 2, mesh.shape["feat"]), ROWS_FEAT)
    specs = (
        P(ROWS_FEAT, None),
        P(ROWS_FEAT, None),
        P("feat", None, None),
        P("feat", None),
        P("feat", None, None),
        P(),
    )
    return jax.shard_map(
        body, mesh=finer, in_specs=specs, out_specs=(P(ROWS_FEAT, None), P()), check_vma=False
    )
```

```python
import functools

import jax
import jax.numpy as jnp
from jax import lax
from jax.experimental import pallas as pl
from jax.experimental.pallas import tpu as pltpu
from jax.sharding import Mesh
from jax.sharding import PartitionSpec as P

ROWS = ("z", "x", "core")
ROWS_FEAT = ("z", "x", "core", "feat")
HIGHEST = lax.Precision.HIGHEST
F32 = jnp.float32
BF16 = jnp.bfloat16

root_two = 1.4142135623730951
penalty = 0.05

LANES = 128
CHUNK = 20
PHASE_ROW = 440
WEIGHT_ROW = 448
BLOCK_ROWS = 640
EXTRA = 152
HALF = 3072

INTERPRET = False


def call(kernel, out_shape, *args, scalars=0, scratch=(), mib=12):
    specs = [pl.BlockSpec(memory_space=pltpu.SMEM)] * scalars
    specs += [pl.BlockSpec(memory_space=pltpu.VMEM)] * (len(args) - scalars)
    outs = jax.tree.map(lambda _: pl.BlockSpec(memory_space=pltpu.VMEM), out_shape)
    return pl.pallas_call(
        kernel,
        out_shape=out_shape,
        in_specs=specs,
        out_specs=outs,
        scratch_shapes=list(scratch),
        compiler_params=pltpu.CompilerParams(vmem_limit_bytes=mib * 2**20),
        interpret=INTERPRET,
    )(*args)


def rows_of(count):
    return jax.ShapeDtypeStruct((count, LANES), F32)


def shifted(x, axis, by):
    size = lax.axis_size(axis)
    return lax.ppermute(x, axis, [(i, (i + by) % size) for i in range(size)])


PLANE = ("x", "feat")


def exchanged(x, axis):
    return lax.all_to_all(x, axis, split_axis=0, concat_axis=0, tiled=True)


def repeated(x, count):
    def kernel(x_ref, out_ref):
        rows = x_ref.shape[0]
        for s in range(count):
            out_ref[s * rows : (s + 1) * rows, :] = x_ref[...]

    return call(kernel, rows_of(count * x.shape[0]), x)


def index_of(axis):
    return lax.axis_index(axis).astype(jnp.int32)


def placed(me, piece, other):
    rows = piece.shape[0]

    def kernel(me_ref, piece_ref, other_ref, out_ref):
        out_ref[pl.ds(pl.multiple_of(me_ref[0] * rows, 8), rows), :] = piece_ref[...]
        out_ref[pl.ds(pl.multiple_of((1 - me_ref[0]) * rows, 8), rows), :] = other_ref[...]

    return call(kernel, rows_of(2 * rows), me.reshape(1), piece, other, scalars=1)


def split(x):
    high = x.astype(BF16)
    rest = x - high.astype(F32)
    middle = rest.astype(BF16)
    return high, middle, (rest - middle.astype(F32)).astype(BF16)


def dot_split(a, b, dim_a, dim_b):
    return lax.dot_general(
        jnp.concatenate([a[n] for n in (2, 0, 1, 1, 0, 0)], axis=dim_a),
        jnp.concatenate([b[n] for n in (0, 2, 1, 0, 1, 0)], axis=dim_b),
        (((dim_a,), (dim_b,)), ((), ())),
        preferred_element_type=F32,
    )


def chunks_of(projections, phases, weights, block_id):
    per_device = projections.shape[0]
    depth, width = projections.shape[1], projections.shape[2]
    outs = weights.shape[2]
    slot = block_id % per_device
    column = (index_of("core") * lax.axis_size("x") + index_of("x")) * LANES
    basis = lax.dynamic_slice(projections, (slot, 0, column), (1, depth, LANES))[0]
    phase = lax.dynamic_slice(phases, (slot, column), (1, LANES))
    old = lax.dynamic_slice(weights, (slot, column, 0), (1, LANES, outs))[0].T
    stacked = jnp.concatenate(
        [
            basis,
            phase,
            jnp.zeros((WEIGHT_ROW - depth - 1, LANES), F32),
            old,
            jnp.zeros((BLOCK_ROWS - WEIGHT_ROW - outs, LANES), F32),
        ]
    )
    size = lax.axis_size("feat")
    return lax.dynamic_slice(
        stacked.reshape(size, BLOCK_ROWS // size, LANES),
        (0, index_of("z") * CHUNK, 0),
        (size, CHUNK, LANES),
    )


def updated_block(projections, phases, weights, block_id):
    axes = ("z", "feat")
    sizes = [lax.axis_size(axis) for axis in axes]
    pieces = chunks_of(projections, phases, weights, block_id)
    pieces = jnp.broadcast_to(pieces, (sizes[0], *pieces.shape)).reshape(-1, CHUNK, LANES)
    pieces = exchanged(pieces, axes).reshape(*sizes, CHUNK, LANES)
    holder = block_id // projections.shape[0]
    part = lax.dynamic_index_in_dim(pieces, holder, 1, False).reshape(-1, LANES)
    part = exchanged(repeated(part, lax.axis_size(PLANE)), PLANE)
    return placed(index_of("core"), part, shifted(part, "core", 1))


def cosine(x):
    turns = jnp.round(x * 0.15915494309189535)
    rest = (x - turns * 6.28125) - turns * 0.0019353071795864769
    sq = rest * rest * 0.25
    c = 2.08767569878681e-09
    for term in (
        -2.755731922398589e-07,
        2.48015873015873e-05,
        -0.001388888888888889,
        0.041666666666666664,
        -0.5,
        1.0,
    ):
        c = c * sq + term
    return 2.0 * (c * c) - 1.0


def products_kernel(core_ref, samples_ref, block_ref, residual_ref, features_ref, keep_ref, send_ref, points, extra, turned, packed):
    blocks = features_ref.shape[0] // LANES
    depth, outs = samples_ref.shape[0], residual_ref.shape[0]
    width = blocks * LANES
    total = width + EXTRA
    points[:depth, :] = samples_ref[...]
    tail = (points.shape[0] - depth, points.shape[1])
    points[depth:, :] = jnp.where(lax.broadcasted_iota(jnp.int32, tail, 0) == PHASE_ROW - depth, 1.0, 0.0)
    for k in range(blocks):
        projected = lax.dot_general(
            block_ref[k * BLOCK_ROWS : k * BLOCK_ROWS + points.shape[0], :],
            points[...],
            (((0,), (0,)), ((), ())),
            precision=HIGHEST,
            preferred_element_type=F32,
        )
        features = root_two * cosine(projected)
        features_ref[k * LANES : (k + 1) * LANES, :] = features
        for n, part in enumerate(split(features)):
            turned[n, k * LANES : (k + 1) * LANES, :] = part
    extra[EXTRA - 8 :, :] = jnp.zeros((8, extra.shape[1]), F32)
    extra[:outs, :] = residual_ref[...]
    for n, part in enumerate(split(extra[...])):
        turned[n, width : width + EXTRA, :] = part
    at = 0
    for k in range(blocks):
        count = total - k * LANES
        packed[at : at + count, :] = dot_split(
            [turned[n, k * LANES : total, :] for n in range(3)],
            [turned[n, k * LANES : (k + 1) * LANES, :] for n in range(3)],
            1,
            1,
        )
        at += count
    packed[at:, :] = jnp.zeros((packed.shape[0] - at, LANES), F32)
    mine = pl.multiple_of(core_ref[0] * HALF, 8)
    theirs = pl.multiple_of((1 - core_ref[0]) * HALF, 8)
    keep_ref[...] = packed[pl.ds(mine, HALF), :]
    send_ref[...] = packed[pl.ds(theirs, HALF), :]


def products(samples, block, residual):
    rows, width = samples.shape[1], block.shape[0] // BLOCK_ROWS * LANES
    return call(
        products_kernel,
        (jax.ShapeDtypeStruct((width, rows), F32), rows_of(HALF), rows_of(HALF)),
        index_of("core").reshape(1),
        samples,
        block,
        residual,
        scalars=1,
        scratch=(
            pltpu.VMEM((WEIGHT_ROW, rows), F32),
            pltpu.VMEM((EXTRA, rows), F32),
            pltpu.VMEM((3, width + EXTRA + 8, rows), BF16),
            pltpu.VMEM((2 * HALF, LANES), F32),
        ),
        mib=24,
    )


def added(a, b):
    def kernel(a_ref, b_ref, out_ref):
        out_ref[...] = a_ref[...] + b_ref[...]

    return call(kernel, rows_of(a.shape[0]), a, b)


def added_parts(x, count):
    rows = x.shape[0] // count

    def kernel(x_ref, out_ref):
        acc = x_ref[:rows, :]
        for s in range(1, count):
            acc = acc + x_ref[s * rows : (s + 1) * rows, :]
        out_ref[...] = acc

    return call(kernel, rows_of(rows), x)


def added_copies(x, count):
    rows = x.shape[0] // count

    def kernel(x_ref, out_ref):
        acc = x_ref[:rows, :]
        for s in range(1, count):
            acc = acc + x_ref[s * rows : (s + 1) * rows, :]
        for s in range(count):
            out_ref[s * rows : (s + 1) * rows, :] = acc

    return call(kernel, rows_of(x.shape[0]), x)


def total_of(keep, send):
    plane, line = lax.axis_size(PLANE), lax.axis_size("z")
    half = added(keep, shifted(send, "core", 1))
    part = added_parts(exchanged(half, PLANE), plane)
    part = exchanged(added_copies(exchanged(part, "z"), line), "z")
    half = exchanged(repeated(part, plane), PLANE)
    return half, shifted(half, "core", 1)


def across_sublanes(tile, row):
    return jnp.broadcast_to(tile[row : row + 1, :], tile.shape)


def columns_of(tile, first):
    return [jnp.broadcast_to(tile[:, first + q : first + q + 1], tile.shape) for q in range(8)]


def inverse_factor(source, target):
    tiles = LANES // 8
    lane = lax.broadcasted_iota(jnp.int32, (8, LANES), 1)
    sub = lax.broadcasted_iota(jnp.int32, (8, LANES), 0)
    rows = [source[8 * v : 8 * v + 8, :] for v in range(tiles)]
    ahead = columns_of(rows[0], 0)
    for b in range(tiles):
        inside = (lane >= 8 * b) & (lane < 8 * b + 8)
        columns = ahead
        tile = jnp.where(inside, jnp.where(lane == 8 * b + sub, 1.0, 0.0), rows[b])
        if b + 1 < tiles:
            ahead = columns_of(rows[b + 1], 8 * b + 8)
        pivots = jnp.ones((8, LANES), F32)
        inverses, multiples, tops = [], [], []
        for q in range(8):
            pivot = across_sublanes(columns[q], q)
            pivots = jnp.where(sub == q, pivot, pivots)
            inverse = 1.0 / pivot
            factor = jnp.where(sub > q, columns[q] * inverse, 0.0)
            multiple = {}
            for later in range(q + 1, 8):
                multiple[later] = across_sublanes(columns[later], q)
                columns[later] = columns[later] - factor * multiple[later]
            top = across_sublanes(tile, q)
            tile = tile - factor * top
            inverses.append(inverse)
            multiples.append(multiple)
            tops.append(top)
        target[8 * b : 8 * b + 8, :] = jnp.where(
            lane <= 8 * b + sub, tile * lax.rsqrt(pivots), 0.0
        )
        for v in range(b + 1, tiles):
            columns = columns_of(rows[v], 8 * b)
            below = jnp.where(inside, 0.0, rows[v])
            for q in range(8):
                factor = columns[q] * inverses[q]
                if v == b + 1:
                    for later in range(8):
                        ahead[later] = ahead[later] - factor * across_sublanes(columns[q], later)
                for later in range(q + 1, 8):
                    columns[later] = columns[later] - factor * multiples[q][later]
                below = below - factor * tops[q]
            rows[v] = below


def solve_kernel(
    total_rows, core_ref, *refs
):
    sums, refs = refs[:2], refs[2:]
    block_ref, features_ref, residual_ref, left_ref, new_ref = refs[:5]
    packed, lower, inverse, corner, raw, right_ref, change_ref = refs[5:]
    outs, rows = residual_ref.shape
    width = features_ref.shape[0]
    blocks = width // LANES
    total = width + EXTRA

    def parts(ref, rows, columns):
        return [ref[n, rows, columns] for n in range(3)]

    for half, ref in zip((core_ref[0], 1 - core_ref[0]), sums):
        packed[pl.ds(pl.multiple_of(half * HALF, 8), HALF), :] = ref[...]
    starts = [k * total - LANES * (k * (k - 1) // 2) for k in range(blocks)]
    diagonal = lax.broadcasted_iota(jnp.int32, (LANES, LANES), 0) == lax.broadcasted_iota(
        jnp.int32, (LANES, LANES), 1
    )

    def step(k, carry):
        for kk in range(blocks):

            @pl.when(k == kk)
            def _():
                here = kk * LANES
                columns = slice(here, here + LANES)
                left = packed[starts[kk] : starts[kk] + total - here, :] * (1.0 / total_rows)
                if kk:
                    left = left - dot_split(
                        parts(lower, slice(here, total), slice(0, here)),
                        parts(lower, columns, slice(0, here)),
                        1,
                        1,
                    )
                corner[...] = left[:LANES] + jnp.where(diagonal, penalty, 0.0)
                if kk < blocks - 1:
                    raw[here + LANES : width, :] = left[LANES : width - here]
                old = block_ref[
                    kk * BLOCK_ROWS + WEIGHT_ROW : kk * BLOCK_ROWS + WEIGHT_ROW + EXTRA, :
                ]
                raw[width:, :] = left[width - here :] - penalty * old

        inverse_factor(corner, inverse.at[k])

        for kk in range(blocks):

            @pl.when(k == kk)
            def _():
                here = kk * LANES
                columns = slice(here, here + LANES)
                below = dot_split(split(raw[here + LANES :, :]), split(inverse[kk]), 1, 1)
                right_ref[:, columns] = below[width - here - LANES :]
                for n, part in enumerate(split(below)):
                    lower[n, here + LANES : total, columns] = part

        return carry

    lax.fori_loop(0, blocks, step, 0)
    for kk in reversed(range(blocks)):
        here = kk * LANES
        columns = slice(here, here + LANES)
        right = right_ref[:, columns]
        if kk < blocks - 1:
            later = slice(here + LANES, width)
            right = right - dot_split(
                parts(change_ref, slice(0, EXTRA), later), parts(lower, later, columns), 1, 0
            )
        change = dot_split(split(right), split(inverse[kk]), 1, 0)
        for n, part in enumerate(split(change)):
            change_ref[n, :EXTRA, columns] = part
        old = block_ref[kk * BLOCK_ROWS + WEIGHT_ROW : kk * BLOCK_ROWS + WEIGHT_ROW + outs, :]
        new_ref[:, 0, columns] = change[:outs] + old
    left_ref[...] = residual_ref[...] - dot_split(
        parts(change_ref, slice(0, EXTRA), slice(0, width)), split(features_ref[...]), 1, 0
    )[:outs]


def solved(sums, block, features, residual, core, total_rows):
    width, rows = features.shape
    outs = residual.shape[0]
    return call(
        functools.partial(solve_kernel, total_rows),
        (
            jax.ShapeDtypeStruct((outs, rows), F32),
            jax.ShapeDtypeStruct((outs, 1, width), F32),
        ),
        core,
        *sums,
        block,
        features,
        residual,
        scalars=1,
        scratch=(
            pltpu.VMEM((2 * HALF, LANES), F32),
            pltpu.VMEM((3, width + EXTRA + 8, width), BF16),
            pltpu.VMEM((width // LANES, LANES, LANES), F32),
            pltpu.VMEM((LANES, LANES), F32),
            pltpu.VMEM((width + EXTRA, LANES), F32),
            pltpu.VMEM((EXTRA, width), F32),
            pltpu.VMEM((3, EXTRA + 8, width), BF16),
        ),
        mib=40,
    )


def body(samples, residual, projections, phases, weights, block_order):
    total_rows = samples.shape[0] * lax.axis_size(ROWS_FEAT)
    residual = residual.T
    block = updated_block(projections, phases, weights, block_order[0])
    features, keep, send = products(samples.T, block, residual)
    sums = total_of(keep, send)
    left, new = solved(
        sums, block, features, residual, index_of("core").reshape(1), total_rows
    )
    return left.T, jnp.transpose(new, (1, 2, 0))


def solution(mesh):
    finer = Mesh(mesh.devices.reshape(8, 4, 2, mesh.shape["feat"]), ROWS_FEAT)
    specs = (
        P(ROWS_FEAT, None),
        P(ROWS_FEAT, None),
        P("feat", None, None),
        P("feat", None),
        P("feat", None, None),
        P(),
    )
    return jax.shard_map(
        body, mesh=finer, in_specs=specs, out_specs=(P(ROWS_FEAT, None), P()), check_vma=False
    )
```
